64 devices in a mesh: inst: 4 (over x, y), qx: 16 (over z, core).
Axes of the slice: x: 2, y: 2, z: 8, core: 2. Of those that a mesh axis runs over, the one named last changes fastest.
The devices are a block of a 4x4x8 slice.
Arguments:
- cost_diag: float32 [4194304], P(('inst', 'qx')), parts along dimension 0
- phase_angles: float32 [6], replicated
- mixer_angles: float32 [6], replicated
Outputs:
- output 1: float32 [4], P('inst'), parts along dimension 0
- output 2: float32 [48], P('inst'), parts along dimension 0
- output 3: float32 [4194304], P(('inst', 'qx')), parts along dimension 0
- output 4: float32 [4194304], P(('inst', 'qx')), parts along dimension 0
There are 4 independent parts. The reference program is written for one: setup_inputs(seed, part) draws one part's arguments, and reference() takes and returns one part's arrays. A program takes and returns all parts, laid end to end along the dimension named above; an argument that names none is the same for every part.
All inputs are finite; a program needn't handle non-finite values.
Results may differ from the reference program's by a relative error of at most 0.001.
Values sent between devices are 32-bit elements.
A program may use at most 768 MiB of HBM per device.

```python
import math
import jax
import jax.numpy as jnp
from jax import lax

STATE_LEN = 1048576
DEGREE = 3
LAYERS = 6
NUM_QUBITS = int(math.log2(STATE_LEN))
NUM_EDGES = NUM_QUBITS * DEGREE // 2


def ising_cost(ends_a, ends_b, weights):
    index = jnp.arange(STATE_LEN, dtype=jnp.int32)

    def add_edge(edge, total):
        bit_a = jnp.right_shift(index, ends_a[edge]) & 1
        bit_b = jnp.right_shift(index, ends_b[edge]) & 1
        spin = (1 - 2 * (bit_a ^ bit_b)).astype(jnp.float32)
        return total + weights[edge] * spin

    total = lax.fori_loop(0, NUM_EDGES, add_edge, jnp.zeros((STATE_LEN,), jnp.float32))
    return total * (NUM_EDGES ** -0.5)


def setup_inputs(seed: int = 0, part: int = 0) -> dict:
    root_key = jax.random.key(seed)
    graph_key = jax.random.fold_in(root_key, part)
    end_key, weight_key = jax.random.split(graph_key)
    ends_a = jnp.arange(NUM_EDGES, dtype=jnp.int32) % NUM_QUBITS
    offsets = jax.random.randint(end_key, (NUM_EDGES,), 1, NUM_QUBITS, dtype=jnp.int32)
    ends_b = (ends_a + offsets) % NUM_QUBITS
    weights = jax.random.uniform(weight_key, (NUM_EDGES,), jnp.float32, 0.5, 1.5)
    cost_diag = ising_cost(ends_a, ends_b, weights)
    gamma_key, beta_key = jax.random.split(jax.random.key(seed + 1))
    phase_angles = jax.random.uniform(gamma_key, (LAYERS,), jnp.float32, 0.2, 0.8)
    mixer_angles = jax.random.uniform(beta_key, (LAYERS,), jnp.float32, 0.4, 1.2)
    return {'cost_diag': cost_diag, 'phase_angles': phase_angles, 'mixer_angles': mixer_angles}


def rotate_pair(state, cos_part, sin_part, partner):
    return cos_part * state + sin_part * jnp.stack([partner[1], -partner[0]])


def apply_mixer(state, cos_half, sin_half):
    for qubit in range(NUM_QUBITS):
        view = state.reshape(2, STATE_LEN >> (qubit + 1), 2, 1 << qubit)
        state = rotate_pair(view, cos_half, sin_half, view[:, :, ::-1, :]).reshape(2, STATE_LEN)
    return state


def undo_mixer(state, adjoint, cos_half, sin_half):
    term = jnp.zeros((), jnp.float32)
    for qubit in range(NUM_QUBITS):
        view_shape = (2, STATE_LEN >> (qubit + 1), 2, 1 << qubit)
        state_view = state.reshape(view_shape)
        adj_view = adjoint.reshape(view_shape)
        state_peer = state_view[:, :, ::-1, :]
        adj_peer = adj_view[:, :, ::-1, :]
        term = term + jnp.sum(adj_view[0] * state_peer[1] - adj_view[1] * state_peer[0])
        state = rotate_pair(state_view, cos_half, -sin_half, state_peer).reshape(2, STATE_LEN)
        adjoint = rotate_pair(adj_view, cos_half, -sin_half, adj_peer).reshape(2, STATE_LEN)
    return state, adjoint, term


def reference(cost_diag, phase_angles, mixer_angles):
    amplitude = 2.0 ** (-NUM_QUBITS / 2)
    start = jnp.stack([jnp.full((STATE_LEN,), amplitude, jnp.float32), jnp.zeros((STATE_LEN,), jnp.float32)])

    def forward_layer(state, angles):
        gamma_now, beta_now = angles
        theta = gamma_now * cost_diag
        state = rotate_pair(state, jnp.cos(theta), jnp.sin(theta), state)
        state = apply_mixer(state, jnp.cos(beta_now / 2), jnp.sin(beta_now / 2))
        return state, None

    final, _ = lax.scan(forward_layer, start, (phase_angles, mixer_angles))
    energy = jnp.sum(cost_diag * (final[0] * final[0] + final[1] * final[1]))

    def backward_layer(carry, angles):
        state, adjoint = carry
        gamma_now, beta_now = angles
        state, adjoint, beta_term = undo_mixer(state, adjoint, jnp.cos(beta_now / 2), jnp.sin(beta_now / 2))
        gamma_term = 2.0 * jnp.sum(cost_diag * (adjoint[0] * state[1] - adjoint[1] * state[0]))
        theta = gamma_now * cost_diag
        cos_phase = jnp.cos(theta)
        sin_phase = jnp.sin(theta)
        state = rotate_pair(state, cos_phase, -sin_phase, state)
        adjoint = rotate_pair(adjoint, cos_phase, -sin_phase, adjoint)
        return (state, adjoint), jnp.stack([gamma_term, beta_term])

    _, terms = lax.scan(backward_layer, (final, cost_diag * final), (phase_angles, mixer_angles), reverse=True)
    gradient = jnp.concatenate([terms[:, 0], terms[:, 1]])
    return energy.reshape(1), gradient, final[0], final[1]
```

```python
import functools
import math

import jax
import jax.numpy as jnp
from jax import lax
from jax.experimental import pallas as pl
from jax.experimental.pallas import tpu as pltpu
from jax.sharding import PartitionSpec as P

LANES = 128
SUBLANES = 8
HALF = SUBLANES // 2
TILES = 8
FEW = TILES // 2
ORDER = (4, 3, 2, 5, 1, 6, 7, 0)
MESH = pl.DeviceIdType.MESH


def bit_count(value, bits):
    total = value & 1
    for bit in range(1, bits):
        total = total + (jnp.right_shift(value, bit) & 1)
    return total


def butterfly(items, tan):
    items = list(items)
    span = 1
    while span < len(items):
        for low in range(len(items)):
            if not low & span:
                first, second = items[low], items[low + span]
                items[low] = first - tan * second
                items[low + span] = second + tan * first
        span *= 2
    return items


def turn(items):
    total = [None] * len(items)
    span = 1
    while span < len(items):
        for low in range(len(items)):
            if not low & span:
                first, second = items[low], items[low + span]
                total[low] = -second if total[low] is None else total[low] - second
                total[low + span] = first if total[low + span] is None else total[low + span] + first
        span *= 2
    return total


def row_index():
    return lax.broadcasted_iota(jnp.int32, (SUBLANES, LANES), 0)


def swap(value):
    return pltpu.roll(value, HALF, 0)


def row_partners(value, bit):
    step = 1 << bit
    down = pltpu.roll(value, step, 0)
    return down, down if 2 * step == SUBLANES else pltpu.roll(value, SUBLANES - step, 0)


def mix_rows(items, tan, bits):
    for bit in range(bits):
        high = jnp.right_shift(row_index(), bit) & 1 == 1
        factor = jnp.where(high, tan, -tan)
        mixed = []
        for item in items:
            down, up = row_partners(item, bit)
            mixed.append(item + factor * (down if down is up else jnp.where(high, down, up)))
        items = mixed
    return items


def turn_rows(items, totals, bits):
    for bit in range(bits):
        high = jnp.right_shift(row_index(), bit) & 1 == 1
        for place, item in enumerate(items):
            down, up = row_partners(item, bit)
            totals[place] = totals[place] + jnp.where(high, down, -up)
    return totals


def flip_lanes(items):
    square = jnp.concatenate(items, axis=0).T
    return [square[place * SUBLANES:(place + 1) * SUBLANES] for place in range(len(items))]


def kernel(layers, groups, qubits, cost_hbm, gamma_hbm, beta_hbm, terms_ref, real_ref, imag_ref,
           cost_ref, gamma_ref, beta_ref, cost_other, tan_buf, scale_buf, cos_buf, sin_buf, start_buf, turn_buf, work_buf,
           mixed_buf, send_buf, recv_buf, adj_buf, adj_send, adj_recv, sums, sums_mine, sums_all,
           send_sem, recv_sem, adj_send_sem, adj_recv_sem, cost_sem, sum_sem, in_sem):
    me = lax.axis_index('qx')
    chips = groups // 2
    chip, core = me // 2, me % 2
    other_core = chip * 2 + 1 - core
    vreg = (SUBLANES, LANES)
    slots = range(groups)
    last = layers - 1
    others = pl.ds(0, groups - 1)
    low_half = row_index() < HALF

    def rows(block):
        return pl.ds(block * SUBLANES, SUBLANES)

    def loop(count, body):
        lax.fori_loop(0, count, lambda step, carry: (body(step), carry)[1], 0)

    def at(step):
        off = ORDER[0]
        for place in range(1, chips):
            off = jnp.where(step == place, ORDER[place], off)
        there = lax.rem(chip + off, chips) * 2
        return [there, there + 1]

    def over_peers(body):
        @functools.partial(loop, chips - 1)
        def _(step):
            for peer in at(step):
                body(peer)

        body(other_core)

    def copy_to(peer, source, target, sends, recvs):
        pltpu.make_async_remote_copy(src_ref=source, dst_ref=target, send_sem=sends, recv_sem=recvs,
                                     device_id={'qx': peer}, device_id_type=MESH).start()

    def drain(view, sem):
        pltpu.make_async_copy(view, view, sem).wait()

    def angles(layer):
        half = jnp.full(vreg, beta_ref[layer], jnp.float32) * 0.5
        cos_half, sin_half = jnp.cos(half), jnp.sin(half)
        tan_buf[layer] = sin_half / cos_half
        scale = cos_half
        for digit in bin(qubits)[3:]:
            scale = scale * scale * (cos_half if digit == '1' else 1.0)
        scale_buf[layer] = scale

    def pack(dense, sign):
        moved = swap(dense)
        return jnp.where(low_half, dense, sign * moved), jnp.where(low_half, moved, sign * dense)

    def phases(layer, costs, scale):
        gamma = gamma_ref[layer]

        @functools.partial(loop, groups)
        def _(slot):
            for block in range(FEW):
                theta = gamma * costs[slot, rows(block)]
                for table, wave, sign in ((cos_buf, jnp.cos, 1.0), (sin_buf, jnp.sin, -1.0)):
                    table[layer, slot, 2 * block], table[layer, slot, 2 * block + 1] = pack(scale * wave(theta), sign)

    def ahead(layer, slot, tile, value):
        start_buf[layer, slot, tile] = value
        return value

    def phase(layer, slot, tile, value):
        return ahead(layer, slot, tile, cos_buf[layer, slot, tile] * value + sin_buf[layer, slot, tile] * swap(value))

    def unphase(layer, slot, tile, value):
        adj_buf[layer, slot, tile] = value
        return cos_buf[layer, slot, tile] * value - sin_buf[layer, slot, tile] * swap(value)

    def mix_slots(source, target, unit, tan):
        @functools.partial(loop, FEW)
        def _(step):
            tile = FEW * unit + step
            for slot, value in enumerate(butterfly([source[slot, tile] for slot in slots], tan)):
                target[slot, tile] = value

    def cross_even(unit, before, between, after):
        @functools.partial(loop, groups // 2)
        def _(step):
            for slot in (2 * step, 2 * step + 1):
                tiles = [FEW * unit + place for place in range(FEW)]
                values = [work_buf[slot, tile] for tile in tiles]
                if before is not None:
                    values = butterfly(values, before)
                values = between(slot, tiles, values)
                if after is not None:
                    for tile, value in zip(tiles, butterfly(values, after)):
                        work_buf[slot, tile] = value

        if after is not None:
            mix_slots(work_buf, mixed_buf, unit, after)

    def cross_odd(source, unit, before, between, after, send):
        tiles = (unit, unit + FEW)
        columns = [butterfly([source[slot, tile] for slot in slots], before) for tile in tiles]
        for slot in slots:
            pair = butterfly([column[slot] for column in columns], before)
            pair = butterfly([between(slot, tile, value) for tile, value in zip(tiles, pair)], after)
            columns[0][slot], columns[1][slot] = pair
        for tile, column in zip(tiles, columns):
            for slot, value in enumerate(butterfly(column, after)):
                send[slot, tile] = value

    def mix_common(peers, tiles, tan, source, send):
        items = [source[peer, tile] for peer in peers for tile in tiles]
        items = flip_lanes(mix_rows(items, tan, 2))
        items = flip_lanes(mix_rows(butterfly(items, tan), tan, 3))
        for place, peer in enumerate(peers):
            for offset, tile in enumerate(tiles):
                send[peer, tile] = items[len(tiles) * place + offset]

    def peers_of(steps, final):
        peers = []
        for step in steps:
            peers += at(2 * step) + at(2 * step + 1)
        peers[-2] = jnp.where(final, other_core, peers[-2])
        peers[-1] = jnp.where(final, me, peers[-1])
        return peers

    def depart_even(layer, unit, tan, send, recv, sends, recvs):
        tiles = [FEW * unit + place for place in range(FEW)]
        steps = chips // 2

        @functools.partial(loop, steps)
        def _(step):
            peers = peers_of([step], step == steps - 1)
            mix_common(peers, tiles, tan, mixed_buf, send)

            def go(peer):
                copy_to(peer, send.at[peer, pl.ds(0, FEW)], recv.at[me, pl.ds(0, FEW)], sends, recvs.at[0])

            @pl.when(unit == 0)
            def _():
                for peer in peers[:-1]:
                    go(peer)

            @pl.when(jnp.logical_and(unit == 0, step < steps - 1))
            def _():
                go(peers[-1])

        for tile in tiles:
            recv[me, tile] = send[me, tile]

        @pl.when(unit == 1)
        def _():
            @functools.partial(loop, FEW)
            def _(place):
                tile = FEW + place
                over_peers(lambda peer: copy_to(peer, send.at[peer, tile], recv.at[me, tile], sends, recvs.at[1 + place]))

    def depart_odd(unit, send, recv, sends, recvs):
        over_peers(lambda peer: copy_to(peer, send.at[peer, unit], recv.at[me, unit], sends, recvs.at[0]))
        for tile in (unit, unit + FEW):
            recv[me, tile] = send[me, tile]

        @pl.when(unit == FEW - 1)
        def _():
            over_peers(lambda peer: copy_to(peer, send.at[peer, pl.ds(FEW, FEW)], recv.at[me, pl.ds(FEW, FEW)], sends, recvs.at[1]))

    def mix_all(unit, tan, state):
        @functools.partial(loop, groups // 8)
        def _(step):
            for part in range(2):
                mix_common([8 * step + 4 * part + place for place in range(4)],
                           [FEW * unit + place for place in range(FEW)], tan, state, state)

    def arrive_even(unit, tan, recv, recvs):
        drain(recv.at[others, pl.ds(0, FEW)], recvs.at[unit])
        mix_all(unit, tan, recv)

    def arrive_odd(unit, recv, recvs):
        @pl.when(unit == 0)
        def _():
            drain(recv.at[others, pl.ds(0, FEW)], recvs.at[0])

        drain(recv.at[others, 0], recvs.at[1 + unit])

    def forward_of(layer):
        return tan_buf[layer], send_buf.at[layer], recv_buf.at[layer], send_sem.at[layer], recv_sem.at[layer]

    def backward_of(layer):
        return -tan_buf[layer], adj_send.at[layer], adj_recv.at[layer], adj_send_sem.at[layer], adj_recv_sem.at[layer]

    def turns(layer):
        @functools.partial(loop, TILES)
        def _(tile):
            for slot, value in enumerate(turn([start_buf[layer, slot, tile] for slot in slots])):
                turn_buf[layer, slot, tile] = value

        @functools.partial(loop, groups // 2)
        def _(step):
            places = [(2 * step + side, tile) for side in range(2) for tile in range(TILES)]
            items = [start_buf[layer, slot, tile] for slot, tile in places]
            totals = turn_rows(items, turn(items[:TILES]) + turn(items[TILES:]), 2)
            items = flip_lanes(items)
            items = flip_lanes(turn_rows(items, turn(items), 3))
            for place, (slot, tile) in enumerate(places):
                turn_buf[layer, slot, tile] = turn_buf[layer, slot, tile] + (totals[place] + items[place])

    over_peers(lambda peer: pl.semaphore_signal(
        pltpu.get_barrier_semaphore(), inc=1, device_id={'qx': peer}, device_id_type=MESH))
    loads = [pltpu.make_async_copy(source, target, in_sem.at[place]) for place, (source, target) in
             enumerate(((beta_hbm, beta_ref), (gamma_hbm, gamma_ref), (cost_hbm, cost_ref)))]
    for load in loads:
        load.start()
    sums_all[...] = jnp.zeros_like(sums_all)

    index_bits = bit_count(row_index() & (HALF - 1), 2) + bit_count(lax.broadcasted_iota(jnp.int32, vreg, 1), 7)
    quarter = (index_bits + bit_count(me, int(math.log2(groups)))) & 3

    def twist(slot, tile):
        now = (quarter + (bit_count(slot, int(math.log2(groups))) + bit_count(tile, 3))) & 3
        return (jnp.where(now == 0, 1.0, jnp.where(now == 2, -1.0, 0.0)),
                jnp.where(now == 1, 1.0, jnp.where(now == 3, -1.0, 0.0)))

    loads[0].wait()
    loop(layers, angles)
    loads[1].wait()
    loads[2].wait()
    phases(0, cost_ref, 2.0 ** (-qubits / 2))
    pl.semaphore_wait(pltpu.get_barrier_semaphore(), groups - 1)
    over_peers(lambda peer: copy_to(peer, cost_ref.at[peer], cost_other.at[me], cost_sem.at[0], cost_sem.at[1]))
    cost_other[me] = cost_ref[me]

    def begin(slot, tiles, values):
        values = []
        for tile in tiles:
            even, odd = twist(slot, tile)
            values.append(ahead(0, slot, tile, jnp.where(low_half, even, odd) * cos_buf[0, slot, tile]
                                + jnp.where(low_half, odd, even) * sin_buf[0, slot, tile]))
        return values

    @functools.partial(loop, 2)
    def _(unit):
        cross_even(unit, None, begin, tan_buf[0])
        depart_even(0, unit, *forward_of(0))

    drain(cost_other.at[others], cost_sem.at[1])
    phases(1, cost_other, scale_buf[0])
    turns(0)

    @functools.partial(loop, layers // 2)
    def _(pair):
        layer = 2 * pair + 1

        @functools.partial(loop, FEW)
        def _(unit):
            arrive_odd(unit, recv_buf.at[layer - 1], recv_sem.at[layer - 1])
            tan, *routes = forward_of(layer)
            cross_odd(recv_buf.at[layer - 1], unit, tan_buf[layer - 1], functools.partial(phase, layer), tan, routes[0])
            depart_odd(unit, *routes)

        @pl.when(layer < last)
        def _():
            phases(layer + 1, cost_ref, scale_buf[layer])

        turns(layer)

        @pl.when(layer < last)
        def _():
            even = layer + 1

            @functools.partial(loop, 2)
            def _(unit):
                arrive_even(unit, tan_buf[layer], recv_buf.at[layer], recv_sem.at[layer])
                mix_slots(recv_buf.at[layer], work_buf, unit, tan_buf[layer])
                cross_even(unit, tan_buf[layer], lambda slot, tiles, values: [
                    phase(even, slot, tile, value) for tile, value in zip(tiles, values)], tan_buf[even])
                depart_even(even, unit, *forward_of(even))

            phases(even + 1, cost_other, scale_buf[even])
            turns(even)

    sums[0] = jnp.zeros(vreg, jnp.float32)

    def middle(slot, tiles, values):
        scale = scale_buf[last]
        values = [scale * value for value in values]
        energy = sums[0]
        adjoint = []
        for pair in range(FEW // 2):
            block = tiles[2 * pair] // 2
            dense = pl.ds(pl.multiple_of(block * SUBLANES, SUBLANES), SUBLANES)
            final = []
            for tile, value in zip(tiles[2 * pair:2 * pair + 2], values[2 * pair:2 * pair + 2]):
                even, odd = twist(slot, tile)
                final.append(even * value + jnp.where(low_half, odd, -odd) * swap(value))
            real_ref[slot, dense] = jnp.where(low_half, final[0], swap(final[1]))
            imag_ref[slot, dense] = jnp.where(low_half, swap(final[0]), final[1])
            for cost, value in zip(pack(cost_ref[slot, dense], 1.0), values[2 * pair:2 * pair + 2]):
                turned = cost * value
                energy = energy + turned * value
                adjoint.append(scale * turned)
        sums[0] = energy
        return adjoint

    @functools.partial(loop, 2)
    def _(unit):
        arrive_even(unit, tan_buf[last], recv_buf.at[last], recv_sem.at[last])
        mix_slots(recv_buf.at[last], work_buf, unit, tan_buf[last])
        cross_even(unit, tan_buf[last], middle, -tan_buf[last])
        depart_even(last, unit, *backward_of(last))

    def slot_terms(layer, mixed):
        def one(tile, total):
            for slot, value in enumerate(turn([recv_buf[layer, slot, tile] for slot in slots])):
                total = total + mixed[slot, tile] * value
            return total

        sums[1 + layers + layer] = lax.fori_loop(0, TILES, one, jnp.zeros(vreg, jnp.float32))

    def start_terms(layer, costs):
        def one(slot, carry):
            gamma_sum, beta_sum = carry
            for block in range(FEW):
                for tile, cost in zip((2 * block, 2 * block + 1), pack(costs[slot, rows(block)], -1.0)):
                    adjoint = adj_buf[layer, slot, tile]
                    gamma_sum = gamma_sum + cost * (adjoint * swap(start_buf[layer, slot, tile]))
                    beta_sum = beta_sum + adjoint * turn_buf[layer, slot, tile]
            return gamma_sum, beta_sum

        zero = jnp.zeros(vreg, jnp.float32)
        gamma_sum, beta_sum = lax.fori_loop(0, groups, one, (zero, zero))
        sums[1 + layer] = 2.0 * gamma_sum
        sums[1 + layers + layer] = sums[1 + layers + layer] + beta_sum

    slot_terms(last, mixed_buf)

    @functools.partial(loop, groups)
    def _(slot):
        for block in range(FEW):
            for tile, cost in zip((2 * block, 2 * block + 1), pack(cost_ref[slot, rows(block)], -1.0)):
                adj_buf[0, slot, tile] = (2.0 * cost) * swap(start_buf[0, slot, tile])

    for state in (adj_buf.at[0], turn_buf.at[0]):
        @functools.partial(loop, 2)
        def _(unit):
            mix_all(unit, tan_buf[0], state)
            mix_slots(state, state, unit, tan_buf[0])

            @functools.partial(loop, groups)
            def _(slot):
                tiles = [FEW * unit + place for place in range(FEW)]
                for tile, value in zip(tiles, butterfly([state[slot, tile] for tile in tiles], tan_buf[0])):
                    state[slot, tile] = value


    @functools.partial(loop, layers // 2)
    def _(pair):
        layer = last - 2 * pair

        @functools.partial(loop, FEW)
        def _(unit):
            arrive_odd(unit, adj_recv.at[layer], adj_recv_sem.at[layer])
            tan, *routes = backward_of(layer - 1)
            cross_odd(adj_recv.at[layer], unit, -tan_buf[layer], functools.partial(unphase, layer), tan, routes[0])
            depart_odd(unit, *routes)

        slot_terms(layer - 1, adj_send.at[layer - 1])
        start_terms(layer, cost_other)

        @pl.when(layer > 1)
        def _():
            even = layer - 1

            @functools.partial(loop, 2)
            def _(unit):
                arrive_even(unit, -tan_buf[even], adj_recv.at[even], adj_recv_sem.at[even])
                mix_slots(adj_recv.at[even], work_buf, unit, -tan_buf[even])
                cross_even(unit, -tan_buf[even], lambda slot, tiles, values: [
                    unphase(even, slot, tile, value) for tile, value in zip(tiles, values)], -tan_buf[even - 1])
                depart_even(even - 1, unit, *backward_of(even - 1))

            slot_terms(even - 1, mixed_buf)
            start_terms(even, cost_ref)

    sums[1] = jnp.zeros(vreg, jnp.float32)

    def meet(unit):
        drain(adj_recv.at[0, others, pl.ds(0, FEW)], adj_recv_sem.at[0, unit])

        def one(slot, carry):
            gamma_sums, beta_sums = list(carry[:FEW]), list(carry[FEW:])
            for place in range(FEW):
                adjoint = adj_recv[0, slot, FEW * unit + place]
                gamma_sums[place] = gamma_sums[place] + adjoint * adj_buf[0, slot, FEW * unit + place]
                beta_sums[place] = beta_sums[place] + adjoint * turn_buf[0, slot, FEW * unit + place]
            return tuple(gamma_sums + beta_sums)

        values = lax.fori_loop(0, groups, one, tuple(jnp.zeros(vreg, jnp.float32) for _ in range(2 * FEW)))
        for term, parts in ((1, values[:FEW]), (1 + layers, values[FEW:])):
            sums[term] = sums[term] + ((parts[0] + parts[1]) + (parts[2] + parts[3]))

    lane = lax.broadcasted_iota(jnp.int32, vreg, 1)

    def gather(terms, mine):
        for term in terms:
            total = jnp.sum(jnp.sum(sums[term], axis=1, keepdims=True), axis=0, keepdims=True)
            place = jnp.logical_and(lane == max(term - 1, 0), row_index() == int(term == 0))
            mine = jnp.where(place, total, mine)
        return mine

    meet(0)
    late = (1, 1 + layers)
    sums_mine[...] = gather([term for term in range(1 + 2 * layers) if term not in late], jnp.zeros(vreg, jnp.float32))
    meet(1)
    mine = gather(late, sums_mine[...])
    sums_mine[...] = mine
    two = pl.ds(0, 2)
    over_peers(lambda peer: copy_to(peer, sums_mine.at[two], sums_all.at[me, two], sum_sem.at[0], sum_sem.at[1]))
    drain(sums_all.at[others, two], sum_sem.at[1])
    total = jnp.zeros(vreg, jnp.float32)
    for slot in slots:
        total = total + jnp.where(slot == me, mine, sums_all[slot])
    terms_ref[...] = total

    drain(cost_other.at[others], cost_sem.at[0])
    drain(sums_all.at[others, two], sum_sem.at[0])

    @functools.partial(loop, layers)
    def _(layer):
        drain(send_buf.at[layer, others], send_sem.at[layer])
        drain(adj_send.at[layer, others], adj_send_sem.at[layer])


def finish(terms_ref, real_in, imag_in, energy_ref, grad_ref, real_ref, imag_ref, energy_buf, grad_buf, sems):
    copies = [pltpu.make_async_copy(source, target, sems.at[place]) for place, (source, target) in enumerate((
        (real_in, real_ref), (imag_in, imag_ref), (energy_buf, energy_ref), (grad_buf, grad_ref)))]
    copies[0].start()
    copies[1].start()
    grad_buf[...] = terms_ref[0, :grad_buf.shape[0]]
    energy_buf[...] = terms_ref[1, :1]
    copies[2].start()
    copies[3].start()
    for copy in copies:
        copy.wait()


def solution(mesh):
    groups = mesh.shape['qx']

    def per_device(cost_flat, phase_angles, mixer_angles):
        chunk_len = cost_flat.shape[0]
        layers = phase_angles.shape[0]
        slot_rows = chunk_len // (groups * LANES)
        assert slot_rows == TILES * HALF and layers % 2 == 0 and groups == 2 * SUBLANES
        qubits = int(math.log2(chunk_len * groups))
        slots = (groups, slot_rows, LANES)
        vreg = (SUBLANES, LANES)
        state = (groups, TILES) + vreg
        states = (layers,) + state
        f32 = jnp.float32
        vmem = pl.BlockSpec(memory_space=pltpu.VMEM)
        hbm = pl.BlockSpec(memory_space=pltpu.HBM)
        dma = pltpu.SemaphoreType.DMA
        shape_of = jax.ShapeDtypeStruct
        results = pl.pallas_call(
            functools.partial(kernel, layers, groups, qubits),
            name='qaoa',
            out_shape=[shape_of(vreg, f32), shape_of(slots, f32), shape_of(slots, f32)],
            in_specs=[hbm] * 3,
            out_specs=[vmem] * 3,
            scratch_shapes=[
                pltpu.VMEM(slots, f32),
                pltpu.SMEM((layers,), f32),
                pltpu.SMEM((layers,), f32),
                pltpu.VMEM(slots, f32),
                pltpu.VMEM((layers,) + vreg, f32),
                pltpu.VMEM((layers,) + vreg, f32),
                pltpu.VMEM(states, f32),
                pltpu.VMEM(states, f32),
                pltpu.VMEM(states, f32),
                pltpu.VMEM(states, f32),
                pltpu.VMEM(state, f32),
                pltpu.VMEM(state, f32),
                pltpu.VMEM(states, f32),
                pltpu.VMEM(states, f32),
                pltpu.VMEM(states, f32),
                pltpu.VMEM(states, f32),
                pltpu.VMEM(states, f32),
                pltpu.VMEM((1 + 2 * layers,) + vreg, f32),
                pltpu.VMEM(vreg, f32),
                pltpu.VMEM((groups,) + vreg, f32),
                dma((layers,)), dma((layers, 1 + FEW)), dma((layers,)), dma((layers, 1 + FEW)),
                dma((2,)), dma((2,)), dma((3,)),
            ],
            compiler_params=pltpu.CompilerParams(
                collective_id=0, has_side_effects=True, vmem_limit_bytes=34 * 1024 * 1024),
        )(*(pltpu.with_memory_space_constraint(value, pltpu.HBM)
            for value in (cost_flat.reshape(slots), phase_angles, mixer_angles)))
        energy, grad, real, imag = pl.pallas_call(
            finish,
            name='finish',
            out_shape=[shape_of((1,), f32), shape_of((2 * layers,), f32), shape_of(slots, f32), shape_of(slots, f32)],
            in_specs=[vmem] * 3,
            out_specs=[hbm] * 4,
            scratch_shapes=[pltpu.VMEM((1,), f32), pltpu.VMEM((2 * layers,), f32), dma((4,))],
            compiler_params=pltpu.CompilerParams(vmem_limit_bytes=2 * 1024 * 1024),
        )(*results)
        return energy, grad, real.reshape(chunk_len), imag.reshape(chunk_len)

    return jax.shard_map(
        per_device, mesh=mesh, in_specs=(P(('inst', 'qx')), P(), P()),
        out_specs=(P('inst'), P('inst'), P(('inst', 'qx')), P(('inst', 'qx'))), check_vma=False)
```

```python
import functools
import math

import jax
import jax.numpy as jnp
from jax import lax
from jax.experimental import pallas as pl
from jax.experimental.pallas import tpu as pltpu
from jax.sharding import PartitionSpec as P

LANES = 128
SUBLANES = 8
HALF = SUBLANES // 2
TILES = 8
FEW = TILES // 2
ORDER = (4, 3, 2, 5, 1, 6, 7, 0)
MESH = pl.DeviceIdType.MESH


def bit_count(value, bits):
    total = value & 1
    for bit in range(1, bits):
        total = total + (jnp.right_shift(value, bit) & 1)
    return total


def butterfly(items, tan):
    items = list(items)
    span = 1
    while span < len(items):
        for low in range(len(items)):
            if not low & span:
                first, second = items[low], items[low + span]
                items[low] = first - tan * second
                items[low + span] = second + tan * first
        span *= 2
    return items


def turn(items):
    total = [None] * len(items)
    span = 1
    while span < len(items):
        for low in range(len(items)):
            if not low & span:
                first, second = items[low], items[low + span]
                total[low] = -second if total[low] is None else total[low] - second
                total[low + span] = first if total[low + span] is None else total[low + span] + first
        span *= 2
    return total


def row_index():
    return lax.broadcasted_iota(jnp.int32, (SUBLANES, LANES), 0)


def swap(value):
    return pltpu.roll(value, HALF, 0)


def row_partners(value, bit):
    step = 1 << bit
    down = pltpu.roll(value, step, 0)
    return down, down if 2 * step == SUBLANES else pltpu.roll(value, SUBLANES - step, 0)


def mix_rows(items, tan, bits):
    for bit in range(bits):
        high = jnp.right_shift(row_index(), bit) & 1 == 1
        factor = jnp.where(high, tan, -tan)
        mixed = []
        for item in items:
            down, up = row_partners(item, bit)
            mixed.append(item + factor * (down if down is up else jnp.where(high, down, up)))
        items = mixed
    return items


def turn_rows(items, totals, bits):
    for bit in range(bits):
        high = jnp.right_shift(row_index(), bit) & 1 == 1
        for place, item in enumerate(items):
            down, up = row_partners(item, bit)
            totals[place] = totals[place] + jnp.where(high, down, -up)
    return totals


def flip_lanes(items):
    square = jnp.concatenate(items, axis=0).T
    return [square[place * SUBLANES:(place + 1) * SUBLANES] for place in range(len(items))]


def kernel(layers, groups, qubits, cost_hbm, gamma_hbm, beta_hbm, terms_ref, real_ref, imag_ref,
           cost_ref, gamma_ref, beta_ref, cost_other, tan_buf, scale_buf, cos_buf, sin_buf, start_buf, turn_buf, work_buf,
           mixed_buf, send_buf, recv_buf, adj_buf, adj_send, adj_recv, sums, sums_mine, sums_all,
           send_sem, recv_sem, adj_send_sem, adj_recv_sem, cost_sem, sum_sem, in_sem):
    me = lax.axis_index('qx')
    chips = groups // 2
    chip, core = me // 2, me % 2
    other_core = chip * 2 + 1 - core
    vreg = (SUBLANES, LANES)
    slots = range(groups)
    last = layers - 1
    others = pl.ds(0, groups - 1)
    low_half = row_index() < HALF

    def rows(block):
        return pl.ds(block * SUBLANES, SUBLANES)

    def loop(count, body):
        lax.fori_loop(0, count, lambda step, carry: (body(step), carry)[1], 0)

    def at(step):
        off = ORDER[0]
        for place in range(1, chips):
            off = jnp.where(step == place, ORDER[place], off)
        there = lax.rem(chip + off, chips) * 2
        return [there, there + 1]

    def over_peers(body):
        @functools.partial(loop, chips - 1)
        def _(step):
            for peer in at(step):
                body(peer)

        body(other_core)

    def copy_to(peer, source, target, sends, recvs):
        pltpu.make_async_remote_copy(src_ref=source, dst_ref=target, send_sem=sends, recv_sem=recvs,
                                     device_id={'qx': peer}, device_id_type=MESH).start()

    def drain(view, sem):
        pltpu.make_async_copy(view, view, sem).wait()

    def angles(layer):
        half = jnp.full(vreg, beta_ref[layer], jnp.float32) * 0.5
        cos_half, sin_half = jnp.cos(half), jnp.sin(half)
        tan_buf[layer] = sin_half / cos_half
        scale = cos_half
        for digit in bin(qubits)[3:]:
            scale = scale * scale * (cos_half if digit == '1' else 1.0)
        scale_buf[layer] = scale

    def pack(dense, sign):
        moved = swap(dense)
        return jnp.where(low_half, dense, sign * moved), jnp.where(low_half, moved, sign * dense)

    def phases(layer, costs, scale):
        gamma = gamma_ref[layer]

        @functools.partial(loop, groups)
        def _(slot):
            for block in range(FEW):
                theta = gamma * costs[slot, rows(block)]
                for table, wave, sign in ((cos_buf, jnp.cos, 1.0), (sin_buf, jnp.sin, -1.0)):
                    table[layer, slot, 2 * block], table[layer, slot, 2 * block + 1] = pack(scale * wave(theta), sign)

    def ahead(layer, slot, tile, value):
        start_buf[layer, slot, tile] = value
        return value

    def phase(layer, slot, tile, value):
        return ahead(layer, slot, tile, cos_buf[layer, slot, tile] * value + sin_buf[layer, slot, tile] * swap(value))

    def unphase(layer, slot, tile, value):
        adj_buf[layer, slot, tile] = value
        return cos_buf[layer, slot, tile] * value - sin_buf[layer, slot, tile] * swap(value)

    def mix_slots(source, target, unit, tan):
        @functools.partial(loop, FEW)
        def _(step):
            tile = FEW * unit + step
            for slot, value in enumerate(butterfly([source[slot, tile] for slot in slots], tan)):
                target[slot, tile] = value

    def cross_even(unit, before, between, after):
        @functools.partial(loop, groups // 2)
        def _(step):
            for slot in (2 * step, 2 * step + 1):
                tiles = [FEW * unit + place for place in range(FEW)]
                values = [work_buf[slot, tile] for tile in tiles]
                if before is not None:
                    values = butterfly(values, before)
                values = between(slot, tiles, values)
                if after is not None:
                    for tile, value in zip(tiles, butterfly(values, after)):
                        work_buf[slot, tile] = value

        if after is not None:
            mix_slots(work_buf, mixed_buf, unit, after)

    def cross_odd(source, unit, before, between, after):
        tiles = (unit, unit + FEW)
        columns = [butterfly([source[slot, tile] for slot in slots], before) for tile in tiles]
        for slot in slots:
            pair = butterfly([column[slot] for column in columns], before)
            pair = butterfly([between(slot, tile, value) for tile, value in zip(tiles, pair)], after)
            columns[0][slot], columns[1][slot] = pair
        for tile, column in zip(tiles, columns):
            for slot, value in enumerate(butterfly(column, after)):
                mixed_buf[slot, tile] = value

    def mix_common(peers, tiles, tan, send):
        items = [mixed_buf[peer, tile] for peer in peers for tile in tiles]
        items = flip_lanes(mix_rows(items, tan, 2))
        items = flip_lanes(mix_rows(butterfly(items, tan), tan, 3))
        for place, peer in enumerate(peers):
            for offset, tile in enumerate(tiles):
                send[peer, tile] = items[len(tiles) * place + offset]

    def peers_of(steps, final):
        peers = []
        for step in steps:
            peers += at(2 * step) + at(2 * step + 1)
        peers[-2] = jnp.where(final, other_core, peers[-2])
        peers[-1] = jnp.where(final, me, peers[-1])
        return peers

    def depart_even(layer, unit, tan, send, recv, sends, recvs):
        tiles = [FEW * unit + place for place in range(FEW)]
        steps = chips // 2

        @functools.partial(loop, steps)
        def _(step):
            peers = peers_of([step], step == steps - 1)
            mix_common(peers, tiles, tan, send)

            def go(peer):
                copy_to(peer, send.at[peer, pl.ds(0, FEW)], recv.at[me, pl.ds(0, FEW)], sends, recvs.at[0])

            @pl.when(unit == 0)
            def _():
                for peer in peers[:-1]:
                    go(peer)

            @pl.when(jnp.logical_and(unit == 0, step < steps - 1))
            def _():
                go(peers[-1])

        for tile in tiles:
            recv[me, tile] = send[me, tile]

        @pl.when(unit == 1)
        def _():
            @functools.partial(loop, FEW)
            def _(place):
                tile = FEW + place
                over_peers(lambda peer: copy_to(peer, send.at[peer, tile], recv.at[me, tile], sends, recvs.at[1 + place]))

    def depart_odd(layer, unit, tan, send, recv, sends, recvs):
        tiles = (unit, unit + FEW)
        steps = chips // 4

        @functools.partial(loop, steps)
        def _(step):
            peers = peers_of([2 * step, 2 * step + 1], step == steps - 1)
            mix_common(peers, tiles, tan, send)

            def go(peer):
                copy_to(peer, send.at[peer, unit], recv.at[me, unit], sends, recvs.at[0])

            for peer in peers[:-1]:
                go(peer)

            @pl.when(step < steps - 1)
            def _():
                go(peers[-1])

        for tile in tiles:
            recv[me, tile] = send[me, tile]

        @pl.when(unit == FEW - 1)
        def _():
            over_peers(lambda peer: copy_to(peer, send.at[peer, pl.ds(FEW, FEW)], recv.at[me, pl.ds(FEW, FEW)], sends, recvs.at[1]))

    def arrive_even(unit, recv, recvs):
        drain(recv.at[others, pl.ds(0, FEW)], recvs.at[unit])

    def arrive_odd(unit, recv, recvs):
        @pl.when(unit == 0)
        def _():
            drain(recv.at[others, pl.ds(0, FEW)], recvs.at[0])

        drain(recv.at[others, 0], recvs.at[1 + unit])

    def forward_of(layer):
        return tan_buf[layer], send_buf.at[layer], recv_buf.at[layer], send_sem.at[layer], recv_sem.at[layer]

    def backward_of(layer):
        return -tan_buf[layer], adj_send.at[layer], adj_recv.at[layer], adj_send_sem.at[layer], adj_recv_sem.at[layer]

    def turns(layer):
        @functools.partial(loop, TILES)
        def _(tile):
            for slot, value in enumerate(turn([start_buf[layer, slot, tile] for slot in slots])):
                turn_buf[layer, slot, tile] = value

        @functools.partial(loop, groups // 2)
        def _(step):
            places = [(2 * step + side, tile) for side in range(2) for tile in range(TILES)]
            items = [start_buf[layer, slot, tile] for slot, tile in places]
            totals = turn_rows(items, turn(items[:TILES]) + turn(items[TILES:]), 2)
            items = flip_lanes(items)
            items = flip_lanes(turn_rows(items, turn(items), 3))
            for place, (slot, tile) in enumerate(places):
                turn_buf[layer, slot, tile] = turn_buf[layer, slot, tile] + (totals[place] + items[place])

    over_peers(lambda peer: pl.semaphore_signal(
        pltpu.get_barrier_semaphore(), inc=1, device_id={'qx': peer}, device_id_type=MESH))
    loads = [pltpu.make_async_copy(source, target, in_sem.at[place]) for place, (source, target) in
             enumerate(((beta_hbm, beta_ref), (gamma_hbm, gamma_ref), (cost_hbm, cost_ref)))]
    for load in loads:
        load.start()
    sums_all[...] = jnp.zeros_like(sums_all)

    index_bits = bit_count(row_index() & (HALF - 1), 2) + bit_count(lax.broadcasted_iota(jnp.int32, vreg, 1), 7)
    quarter = (index_bits + bit_count(me, int(math.log2(groups)))) & 3

    def twist(slot, tile):
        now = (quarter + (bit_count(slot, int(math.log2(groups))) + bit_count(tile, 3))) & 3
        return (jnp.where(now == 0, 1.0, jnp.where(now == 2, -1.0, 0.0)),
                jnp.where(now == 1, 1.0, jnp.where(now == 3, -1.0, 0.0)))

    loads[0].wait()
    loop(layers, angles)
    loads[1].wait()
    loads[2].wait()
    phases(0, cost_ref, 2.0 ** (-qubits / 2))
    pl.semaphore_wait(pltpu.get_barrier_semaphore(), groups - 1)
    over_peers(lambda peer: copy_to(peer, cost_ref.at[peer], cost_other.at[me], cost_sem.at[0], cost_sem.at[1]))
    cost_other[me] = cost_ref[me]

    def begin(slot, tiles, values):
        values = []
        for tile in tiles:
            even, odd = twist(slot, tile)
            values.append(ahead(0, slot, tile, jnp.where(low_half, even, odd) * cos_buf[0, slot, tile]
                                + jnp.where(low_half, odd, even) * sin_buf[0, slot, tile]))
        return values

    @functools.partial(loop, 2)
    def _(unit):
        cross_even(unit, None, begin, tan_buf[0])
        depart_even(0, unit, *forward_of(0))

    drain(cost_other.at[others], cost_sem.at[1])
    phases(1, cost_other, scale_buf[0])
    turns(0)

    @functools.partial(loop, layers // 2)
    def _(pair):
        layer = 2 * pair + 1

        @functools.partial(loop, FEW)
        def _(unit):
            arrive_odd(unit, recv_buf.at[layer - 1], recv_sem.at[layer - 1])
            cross_odd(recv_buf.at[layer - 1], unit, tan_buf[layer - 1], functools.partial(phase, layer), tan_buf[layer])
            depart_odd(layer, unit, *forward_of(layer))

        @pl.when(layer < last)
        def _():
            phases(layer + 1, cost_ref, scale_buf[layer])

        turns(layer)

        @pl.when(layer < last)
        def _():
            even = layer + 1

            @functools.partial(loop, 2)
            def _(unit):
                arrive_even(unit, recv_buf.at[layer], recv_sem.at[layer])
                mix_slots(recv_buf.at[layer], work_buf, unit, tan_buf[layer])
                cross_even(unit, tan_buf[layer], lambda slot, tiles, values: [
                    phase(even, slot, tile, value) for tile, value in zip(tiles, values)], tan_buf[even])
                depart_even(even, unit, *forward_of(even))

            phases(even + 1, cost_other, scale_buf[even])
            turns(even)

    sums[0] = jnp.zeros(vreg, jnp.float32)

    def middle(slot, tiles, values):
        scale = scale_buf[last]
        values = [scale * value for value in values]
        energy = sums[0]
        adjoint = []
        for pair in range(FEW // 2):
            block = tiles[2 * pair] // 2
            dense = pl.ds(pl.multiple_of(block * SUBLANES, SUBLANES), SUBLANES)
            final = []
            for tile, value in zip(tiles[2 * pair:2 * pair + 2], values[2 * pair:2 * pair + 2]):
                even, odd = twist(slot, tile)
                final.append(even * value + jnp.where(low_half, odd, -odd) * swap(value))
            real_ref[slot, dense] = jnp.where(low_half, final[0], swap(final[1]))
            imag_ref[slot, dense] = jnp.where(low_half, swap(final[0]), final[1])
            for cost, value in zip(pack(cost_ref[slot, dense], 1.0), values[2 * pair:2 * pair + 2]):
                turned = cost * value
                energy = energy + turned * value
                adjoint.append(scale * turned)
        sums[0] = energy
        return adjoint

    @functools.partial(loop, 2)
    def _(unit):
        arrive_even(unit, recv_buf.at[last], recv_sem.at[last])
        mix_slots(recv_buf.at[last], work_buf, unit, tan_buf[last])
        cross_even(unit, tan_buf[last], middle, -tan_buf[last])
        depart_even(last, unit, *backward_of(last))

    def slot_terms(layer):
        def one(tile, total):
            for slot, value in enumerate(turn([recv_buf[layer, slot, tile] for slot in slots])):
                total = total + mixed_buf[slot, tile] * value
            return total

        sums[1 + layers + layer] = lax.fori_loop(0, TILES, one, jnp.zeros(vreg, jnp.float32))

    def start_terms(layer, costs):
        def one(slot, carry):
            gamma_sum, beta_sum = carry
            for block in range(FEW):
                for tile, cost in zip((2 * block, 2 * block + 1), pack(costs[slot, rows(block)], -1.0)):
                    adjoint = adj_buf[layer, slot, tile]
                    gamma_sum = gamma_sum + cost * (adjoint * swap(start_buf[layer, slot, tile]))
                    beta_sum = beta_sum + adjoint * turn_buf[layer, slot, tile]
            return gamma_sum, beta_sum

        zero = jnp.zeros(vreg, jnp.float32)
        gamma_sum, beta_sum = lax.fori_loop(0, groups, one, (zero, zero))
        sums[1 + layer] = 2.0 * gamma_sum
        sums[1 + layers + layer] = sums[1 + layers + layer] + beta_sum

    slot_terms(last)

    @functools.partial(loop, layers // 2)
    def _(pair):
        layer = last - 2 * pair

        @functools.partial(loop, FEW)
        def _(unit):
            arrive_odd(unit, adj_recv.at[layer], adj_recv_sem.at[layer])
            cross_odd(adj_recv.at[layer], unit, -tan_buf[layer], functools.partial(unphase, layer), -tan_buf[layer - 1])
            depart_odd(layer - 1, unit, *backward_of(layer - 1))

        slot_terms(layer - 1)
        start_terms(layer, cost_other)

        @pl.when(layer > 1)
        def _():
            even = layer - 1

            @functools.partial(loop, 2)
            def _(unit):
                arrive_even(unit, adj_recv.at[even], adj_recv_sem.at[even])
                mix_slots(adj_recv.at[even], work_buf, unit, -tan_buf[even])
                cross_even(unit, -tan_buf[even], lambda slot, tiles, values: [
                    unphase(even, slot, tile, value) for tile, value in zip(tiles, values)], -tan_buf[even - 1])
                depart_even(even - 1, unit, *backward_of(even - 1))

            slot_terms(even - 1)
            start_terms(even, cost_ref)

    sums[1] = jnp.zeros(vreg, jnp.float32)

    @functools.partial(loop, groups)
    def _(slot):
        for block in range(FEW):
            for tile, cost in zip((2 * block, 2 * block + 1), pack(cost_ref[slot, rows(block)], -1.0)):
                adj_buf[0, slot, tile] = (2.0 * cost) * swap(start_buf[0, slot, tile])

    for source, target in ((adj_buf.at[0], work_buf), (turn_buf.at[0], mixed_buf)):
        @functools.partial(loop, groups)
        def _(slot):
            for unit in range(2):
                values = butterfly([source[slot, FEW * unit + place] for place in range(FEW)], tan_buf[0])
                for place in range(FEW):
                    source[slot, FEW * unit + place] = values[place]

        for unit in range(2):
            mix_slots(source, target, unit, tan_buf[0])

    def meet(unit):
        arrive_even(unit, adj_recv.at[0], adj_recv_sem.at[0])

        def one(step, carry):
            gamma_sums, beta_sums = list(carry[:FEW]), list(carry[FEW:])
            for slot, place in [(4 * step + side, place) for side in range(4) for place in range(FEW)]:
                adjoint = adj_recv[0, slot, FEW * unit + place]
                gamma_sums[place] = gamma_sums[place] + adjoint * work_buf[slot, FEW * unit + place]
                beta_sums[place] = beta_sums[place] + adjoint * mixed_buf[slot, FEW * unit + place]
            return tuple(gamma_sums + beta_sums)

        values = lax.fori_loop(0, groups // 4, one, tuple(jnp.zeros(vreg, jnp.float32) for _ in range(2 * FEW)))
        for term, parts in ((1, values[:FEW]), (1 + layers, values[FEW:])):
            sums[term] = sums[term] + ((parts[0] + parts[1]) + (parts[2] + parts[3]))

    lane = lax.broadcasted_iota(jnp.int32, vreg, 1)

    def gather(terms, mine):
        for term in terms:
            total = jnp.sum(jnp.sum(sums[term], axis=1, keepdims=True), axis=0, keepdims=True)
            place = jnp.logical_and(lane == max(term - 1, 0), row_index() == int(term == 0))
            mine = jnp.where(place, total, mine)
        return mine

    meet(0)
    late = (1, 1 + layers)
    sums_mine[...] = gather([term for term in range(1 + 2 * layers) if term not in late], jnp.zeros(vreg, jnp.float32))
    meet(1)
    mine = gather(late, sums_mine[...])
    sums_mine[...] = mine
    two = pl.ds(0, 2)
    over_peers(lambda peer: copy_to(peer, sums_mine.at[two], sums_all.at[me, two], sum_sem.at[0], sum_sem.at[1]))
    drain(cost_other.at[others], cost_sem.at[0])

    @functools.partial(loop, layers)
    def _(layer):
        drain(send_buf.at[layer, others], send_sem.at[layer])
        drain(adj_send.at[layer, others], adj_send_sem.at[layer])

    drain(sums_all.at[others, two], sum_sem.at[1])
    totals = [jnp.where(slot == me, mine, sums_all[slot]) for slot in slots]
    while len(totals) > 1:
        totals = [low + high for low, high in zip(totals[0::2], totals[1::2])]
    terms_ref[...] = totals[0]

    drain(sums_all.at[others, two], sum_sem.at[0])


def finish(terms_ref, real_in, imag_in, energy_ref, grad_ref, real_ref, imag_ref, energy_buf, grad_buf, sems):
    copies = [pltpu.make_async_copy(source, target, sems.at[place]) for place, (source, target) in enumerate((
        (real_in, real_ref), (imag_in, imag_ref), (energy_buf, energy_ref), (grad_buf, grad_ref)))]
    copies[0].start()
    copies[1].start()
    grad_buf[...] = terms_ref[0, :grad_buf.shape[0]]
    energy_buf[...] = terms_ref[1, :1]
    copies[2].start()
    copies[3].start()
    for copy in copies:
        copy.wait()


def solution(mesh):
    groups = mesh.shape['qx']

    def per_device(cost_flat, phase_angles, mixer_angles):
        chunk_len = cost_flat.shape[0]
        layers = phase_angles.shape[0]
        slot_rows = chunk_len // (groups * LANES)
        assert slot_rows == TILES * HALF and layers % 2 == 0 and groups == 2 * SUBLANES
        qubits = int(math.log2(chunk_len * groups))
        slots = (groups, slot_rows, LANES)
        vreg = (SUBLANES, LANES)
        state = (groups, TILES) + vreg
        states = (layers,) + state
        f32 = jnp.float32
        vmem = pl.BlockSpec(memory_space=pltpu.VMEM)
        hbm = pl.BlockSpec(memory_space=pltpu.HBM)
        dma = pltpu.SemaphoreType.DMA
        shape_of = jax.ShapeDtypeStruct
        results = pl.pallas_call(
            functools.partial(kernel, layers, groups, qubits),
            name='qaoa',
            out_shape=[shape_of(vreg, f32), shape_of(slots, f32), shape_of(slots, f32)],
            in_specs=[hbm] * 3,
            out_specs=[vmem] * 3,
            scratch_shapes=[
                pltpu.VMEM(slots, f32),
                pltpu.SMEM((layers,), f32),
                pltpu.SMEM((layers,), f32),
                pltpu.VMEM(slots, f32),
                pltpu.VMEM((layers,) + vreg, f32),
                pltpu.VMEM((layers,) + vreg, f32),
                pltpu.VMEM(states, f32),
                pltpu.VMEM(states, f32),
                pltpu.VMEM(states, f32),
                pltpu.VMEM(states, f32),
                pltpu.VMEM(state, f32),
                pltpu.VMEM(state, f32),
                pltpu.VMEM(states, f32),
                pltpu.VMEM(states, f32),
                pltpu.VMEM(states, f32),
                pltpu.VMEM(states, f32),
                pltpu.VMEM(states, f32),
                pltpu.VMEM((1 + 2 * layers,) + vreg, f32),
                pltpu.VMEM(vreg, f32),
                pltpu.VMEM((groups,) + vreg, f32),
                dma((layers,)), dma((layers, 1 + FEW)), dma((layers,)), dma((layers, 1 + FEW)),
                dma((2,)), dma((2,)), dma((3,)),
            ],
            compiler_params=pltpu.CompilerParams(
                collective_id=0, has_side_effects=True, vmem_limit_bytes=34 * 1024 * 1024),
        )(*(pltpu.with_memory_space_constraint(value, pltpu.HBM)
            for value in (cost_flat.reshape(slots), phase_angles, mixer_angles)))
        energy, grad, real, imag = pl.pallas_call(
            finish,
            name='finish',
            out_shape=[shape_of((1,), f32), shape_of((2 * layers,), f32), shape_of(slots, f32), shape_of(slots, f32)],
            in_specs=[vmem] * 3,
            out_specs=[hbm] * 4,
            scratch_shapes=[pltpu.VMEM((1,), f32), pltpu.VMEM((2 * layers,), f32), dma((4,))],
            compiler_params=pltpu.CompilerParams(vmem_limit_bytes=2 * 1024 * 1024),
        )(*results)
        return energy, grad, real.reshape(chunk_len), imag.reshape(chunk_len)

    return jax.shard_map(
        per_device, mesh=mesh, in_specs=(P(('inst', 'qx')), P(), P()),
        out_specs=(P('inst'), P('inst'), P(('inst', 'qx')), P(('inst', 'qx'))), check_vma=False)
```

```python
import functools
import math

import jax
import jax.numpy as jnp
from jax import lax
from jax.experimental import pallas as pl
from jax.experimental.pallas import tpu as pltpu
from jax.sharding import PartitionSpec as P

LANES = 128
SUBLANES = 8
HALF = SUBLANES // 2
TILES = 8
FEW = TILES // 2
ORDER = (4, 3, 2, 5, 1, 6, 7, 0)
MESH = pl.DeviceIdType.MESH


def bit_count(value, bits):
    total = value & 1
    for bit in range(1, bits):
        total = total + (jnp.right_shift(value, bit) & 1)
    return total


def butterfly(items, tan):
    items = list(items)
    span = 1
    while span < len(items):
        for low in range(len(items)):
            if not low & span:
                first, second = items[low], items[low + span]
                items[low] = first - tan * second
                items[low + span] = second + tan * first
        span *= 2
    return items


def turn(items):
    total = [None] * len(items)
    span = 1
    while span < len(items):
        for low in range(len(items)):
            if not low & span:
                first, second = items[low], items[low + span]
                total[low] = -second if total[low] is None else total[low] - second
                total[low + span] = first if total[low + span] is None else total[low + span] + first
        span *= 2
    return total


def row_index():
    return lax.broadcasted_iota(jnp.int32, (SUBLANES, LANES), 0)


def swap(value):
    return pltpu.roll(value, HALF, 0)


def row_partners(value, bit):
    step = 1 << bit
    down = pltpu.roll(value, step, 0)
    return down, down if 2 * step == SUBLANES else pltpu.roll(value, SUBLANES - step, 0)


def mix_rows(items, tan, bits):
    for bit in range(bits):
        high = jnp.right_shift(row_index(), bit) & 1 == 1
        factor = jnp.where(high, tan, -tan)
        mixed = []
        for item in items:
            down, up = row_partners(item, bit)
            mixed.append(item + factor * (down if down is up else jnp.where(high, down, up)))
        items = mixed
    return items


def turn_rows(items, totals, bits):
    for bit in range(bits):
        high = jnp.right_shift(row_index(), bit) & 1 == 1
        for place, item in enumerate(items):
            down, up = row_partners(item, bit)
            totals[place] = totals[place] + jnp.where(high, down, -up)
    return totals


def flip_lanes(items):
    square = jnp.concatenate(items, axis=0).T
    return [square[place * SUBLANES:(place + 1) * SUBLANES] for place in range(len(items))]


def kernel(layers, groups, qubits, cost_hbm, gamma_hbm, beta_hbm, terms_ref, real_ref, imag_ref,
           cost_ref, gamma_ref, beta_ref, cost_other, tan_buf, scale_buf, cos_buf, sin_buf, start_buf, turn_buf, work_buf,
           mixed_buf, send_buf, recv_buf, adj_buf, adj_send, adj_recv, sums, sums_mine, sums_all,
           send_sem, recv_sem, adj_send_sem, adj_recv_sem, cost_sem, sum_sem, in_sem):
    me = lax.axis_index('qx')
    chips = groups // 2
    chip, core = me // 2, me % 2
    other_core = chip * 2 + 1 - core
    vreg = (SUBLANES, LANES)
    slots = range(groups)
    last = layers - 1
    others = pl.ds(0, groups - 1)
    low_half = row_index() < HALF

    def rows(block):
        return pl.ds(block * SUBLANES, SUBLANES)

    def loop(count, body):
        lax.fori_loop(0, count, lambda step, carry: (body(step), carry)[1], 0)

    def at(step):
        off = ORDER[0]
        for place in range(1, chips):
            off = jnp.where(step == place, ORDER[place], off)
        there = lax.rem(chip + off, chips) * 2
        return [there, there + 1]

    def over_peers(body):
        @functools.partial(loop, chips - 1)
        def _(step):
            for peer in at(step):
                body(peer)

        body(other_core)

    def copy_to(peer, source, target, sends, recvs):
        pltpu.make_async_remote_copy(src_ref=source, dst_ref=target, send_sem=sends, recv_sem=recvs,
                                     device_id={'qx': peer}, device_id_type=MESH).start()

    def drain(view, sem):
        pltpu.make_async_copy(view, view, sem).wait()

    def angles(layer):
        half = jnp.full(vreg, beta_ref[layer], jnp.float32) * 0.5
        cos_half, sin_half = jnp.cos(half), jnp.sin(half)
        tan_buf[layer] = sin_half / cos_half
        scale = cos_half
        for digit in bin(qubits)[3:]:
            scale = scale * scale * (cos_half if digit == '1' else 1.0)
        scale_buf[layer] = scale

    def pack(dense, sign):
        moved = swap(dense)
        return jnp.where(low_half, dense, sign * moved), jnp.where(low_half, moved, sign * dense)

    def phases(layer, costs, scale):
        gamma = gamma_ref[layer]

        @functools.partial(loop, groups)
        def _(slot):
            for block in range(FEW):
                theta = gamma * costs[slot, rows(block)]
                for table, wave, sign in ((cos_buf, jnp.cos, 1.0), (sin_buf, jnp.sin, -1.0)):
                    table[layer, slot, 2 * block], table[layer, slot, 2 * block + 1] = pack(scale * wave(theta), sign)

    def ahead(layer, slot, tile, value):
        start_buf[layer, slot, tile] = value
        return value

    def phase(layer, slot, tile, value):
        return ahead(layer, slot, tile, cos_buf[layer, slot, tile] * value + sin_buf[layer, slot, tile] * swap(value))

    def unphase(layer, slot, tile, value):
        adj_buf[layer, slot, tile] = value
        return cos_buf[layer, slot, tile] * value - sin_buf[layer, slot, tile] * swap(value)

    def mix_slots(source, target, unit, tan):
        @functools.partial(loop, FEW)
        def _(step):
            tile = FEW * unit + step
            for slot, value in enumerate(butterfly([source[slot, tile] for slot in slots], tan)):
                target[slot, tile] = value

    def cross_even(unit, before, between, after):
        @functools.partial(loop, groups // 2)
        def _(step):
            for slot in (2 * step, 2 * step + 1):
                tiles = [FEW * unit + place for place in range(FEW)]
                values = [work_buf[slot, tile] for tile in tiles]
                if before is not None:
                    values = butterfly(values, before)
                values = between(slot, tiles, values)
                if after is not None:
                    for tile, value in zip(tiles, butterfly(values, after)):
                        work_buf[slot, tile] = value

        if after is not None:
            mix_slots(work_buf, mixed_buf, unit, after)

    def cross_odd(source, unit, before, between, after):
        tiles = (unit, unit + FEW)
        columns = [butterfly([source[slot, tile] for slot in slots], before) for tile in tiles]
        for slot in slots:
            pair = butterfly([column[slot] for column in columns], before)
            pair = butterfly([between(slot, tile, value) for tile, value in zip(tiles, pair)], after)
            columns[0][slot], columns[1][slot] = pair
        for tile, column in zip(tiles, columns):
            for slot, value in enumerate(butterfly(column, after)):
                mixed_buf[slot, tile] = value

    def mix_common(peers, tiles, tan, send):
        items = [mixed_buf[peer, tile] for peer in peers for tile in tiles]
        items = flip_lanes(mix_rows(items, tan, 2))
        items = flip_lanes(mix_rows(butterfly(items, tan), tan, 3))
        for place, peer in enumerate(peers):
            for offset, tile in enumerate(tiles):
                send[peer, tile] = items[len(tiles) * place + offset]

    def peers_of(steps, final):
        peers = []
        for step in steps:
            peers += at(2 * step) + at(2 * step + 1)
        peers[-2] = jnp.where(final, other_core, peers[-2])
        peers[-1] = jnp.where(final, me, peers[-1])
        return peers

    def depart_even(layer, unit, tan, send, recv, sends, recvs):
        tiles = [FEW * unit + place for place in range(FEW)]
        steps = chips // 2

        @functools.partial(loop, steps)
        def _(step):
            peers = peers_of([step], step == steps - 1)
            mix_common(peers, tiles, tan, send)

            def go(peer):
                copy_to(peer, send.at[peer, pl.ds(0, FEW)], recv.at[me, pl.ds(0, FEW)], sends, recvs.at[0])

            @pl.when(unit == 0)
            def _():
                for peer in peers[:-1]:
                    go(peer)

            @pl.when(jnp.logical_and(unit == 0, step < steps - 1))
            def _():
                go(peers[-1])

        for tile in tiles:
            recv[me, tile] = send[me, tile]

        @pl.when(unit == 1)
        def _():
            @functools.partial(loop, FEW)
            def _(place):
                tile = FEW + place
                over_peers(lambda peer: copy_to(peer, send.at[peer, tile], recv.at[me, tile], sends, recvs.at[1 + place]))

    def depart_odd(layer, unit, tan, send, recv, sends, recvs):
        tiles = (unit, unit + FEW)
        steps = chips // 4

        @functools.partial(loop, steps)
        def _(step):
            peers = peers_of([2 * step, 2 * step + 1], step == steps - 1)
            mix_common(peers, tiles, tan, send)

            def go(peer):
                copy_to(peer, send.at[peer, unit], recv.at[me, unit], sends, recvs.at[0])

            for peer in peers[:-1]:
                go(peer)

            @pl.when(step < steps - 1)
            def _():
                go(peers[-1])

        for tile in tiles:
            recv[me, tile] = send[me, tile]

        @pl.when(unit == FEW - 1)
        def _():
            over_peers(lambda peer: copy_to(peer, send.at[peer, pl.ds(FEW, FEW)], recv.at[me, pl.ds(FEW, FEW)], sends, recvs.at[1]))

    def arrive_even(unit, recv, recvs):
        drain(recv.at[others, pl.ds(0, FEW)], recvs.at[unit])

    def arrive_odd(unit, recv, recvs):
        @pl.when(unit == 0)
        def _():
            drain(recv.at[others, pl.ds(0, FEW)], recvs.at[0])

        drain(recv.at[others, 0], recvs.at[1 + unit])

    def forward_of(layer):
        return tan_buf[layer], send_buf.at[layer], recv_buf.at[layer], send_sem.at[layer], recv_sem.at[layer]

    def backward_of(layer):
        return -tan_buf[layer], adj_send.at[layer], adj_recv.at[layer], adj_send_sem.at[layer], adj_recv_sem.at[layer]

    def turns(layer):
        @functools.partial(loop, TILES)
        def _(tile):
            for slot, value in enumerate(turn([start_buf[layer, slot, tile] for slot in slots])):
                turn_buf[layer, slot, tile] = value

        @functools.partial(loop, groups // 2)
        def _(step):
            places = [(2 * step + side, tile) for side in range(2) for tile in range(TILES)]
            items = [start_buf[layer, slot, tile] for slot, tile in places]
            totals = turn_rows(items, turn(items[:TILES]) + turn(items[TILES:]), 2)
            items = flip_lanes(items)
            items = flip_lanes(turn_rows(items, turn(items), 3))
            for place, (slot, tile) in enumerate(places):
                turn_buf[layer, slot, tile] = turn_buf[layer, slot, tile] + (totals[place] + items[place])

    over_peers(lambda peer: pl.semaphore_signal(
        pltpu.get_barrier_semaphore(), inc=1, device_id={'qx': peer}, device_id_type=MESH))
    loads = [pltpu.make_async_copy(source, target, in_sem.at[place]) for place, (source, target) in
             enumerate(((beta_hbm, beta_ref), (gamma_hbm, gamma_ref), (cost_hbm, cost_ref)))]
    for load in loads:
        load.start()
    sums_all[...] = jnp.zeros_like(sums_all)

    index_bits = bit_count(row_index() & (HALF - 1), 2) + bit_count(lax.broadcasted_iota(jnp.int32, vreg, 1), 7)
    quarter = (index_bits + bit_count(me, int(math.log2(groups)))) & 3

    def twist(slot, tile):
        now = (quarter + (bit_count(slot, int(math.log2(groups))) + bit_count(tile, 3))) & 3
        return (jnp.where(now == 0, 1.0, jnp.where(now == 2, -1.0, 0.0)),
                jnp.where(now == 1, 1.0, jnp.where(now == 3, -1.0, 0.0)))

    loads[0].wait()
    loop(layers, angles)
    loads[1].wait()
    loads[2].wait()
    phases(0, cost_ref, 2.0 ** (-qubits / 2))
    pl.semaphore_wait(pltpu.get_barrier_semaphore(), groups - 1)
    over_peers(lambda peer: copy_to(peer, cost_ref.at[peer], cost_other.at[me], cost_sem.at[0], cost_sem.at[1]))
    cost_other[me] = cost_ref[me]

    def begin(slot, tiles, values):
        values = []
        for tile in tiles:
            even, odd = twist(slot, tile)
            values.append(ahead(0, slot, tile, jnp.where(low_half, even, odd) * cos_buf[0, slot, tile]
                                + jnp.where(low_half, odd, even) * sin_buf[0, slot, tile]))
        return values

    @functools.partial(loop, 2)
    def _(unit):
        cross_even(unit, None, begin, tan_buf[0])
        depart_even(0, unit, *forward_of(0))

    drain(cost_other.at[others], cost_sem.at[1])
    phases(1, cost_other, scale_buf[0])
    turns(0)

    @functools.partial(loop, layers // 2)
    def _(pair):
        layer = 2 * pair + 1

        @functools.partial(loop, FEW)
        def _(unit):
            arrive_odd(unit, recv_buf.at[layer - 1], recv_sem.at[layer - 1])
            cross_odd(recv_buf.at[layer - 1], unit, tan_buf[layer - 1], functools.partial(phase, layer), tan_buf[layer])
            depart_odd(layer, unit, *forward_of(layer))

        @pl.when(layer < last)
        def _():
            phases(layer + 1, cost_ref, scale_buf[layer])

        turns(layer)

        @pl.when(layer < last)
        def _():
            even = layer + 1

            @functools.partial(loop, 2)
            def _(unit):
                arrive_even(unit, recv_buf.at[layer], recv_sem.at[layer])
                mix_slots(recv_buf.at[layer], work_buf, unit, tan_buf[layer])
                cross_even(unit, tan_buf[layer], lambda slot, tiles, values: [
                    phase(even, slot, tile, value) for tile, value in zip(tiles, values)], tan_buf[even])
                depart_even(even, unit, *forward_of(even))

            phases(even + 1, cost_other, scale_buf[even])
            turns(even)

    sums[0] = jnp.zeros(vreg, jnp.float32)

    def middle(slot, tiles, values):
        scale = scale_buf[last]
        values = [scale * value for value in values]
        energy = sums[0]
        adjoint = []
        for pair in range(FEW // 2):
            block = tiles[2 * pair] // 2
            dense = pl.ds(pl.multiple_of(block * SUBLANES, SUBLANES), SUBLANES)
            final = []
            for tile, value in zip(tiles[2 * pair:2 * pair + 2], values[2 * pair:2 * pair + 2]):
                even, odd = twist(slot, tile)
                final.append(even * value + jnp.where(low_half, odd, -odd) * swap(value))
            real_ref[slot, dense] = jnp.where(low_half, final[0], swap(final[1]))
            imag_ref[slot, dense] = jnp.where(low_half, swap(final[0]), final[1])
            for cost, value in zip(pack(cost_ref[slot, dense], 1.0), values[2 * pair:2 * pair + 2]):
                turned = cost * value
                energy = energy + turned * value
                adjoint.append(scale * turned)
        sums[0] = energy
        return adjoint

    @functools.partial(loop, 2)
    def _(unit):
        arrive_even(unit, recv_buf.at[last], recv_sem.at[last])
        mix_slots(recv_buf.at[last], work_buf, unit, tan_buf[last])
        cross_even(unit, tan_buf[last], middle, -tan_buf[last])
        depart_even(last, unit, *backward_of(last))

    def slot_terms(layer):
        def one(tile, total):
            for slot, value in enumerate(turn([recv_buf[layer, slot, tile] for slot in slots])):
                total = total + mixed_buf[slot, tile] * value
            return total

        sums[1 + layers + layer] = lax.fori_loop(0, TILES, one, jnp.zeros(vreg, jnp.float32))

    def start_terms(layer, costs):
        def one(slot, carry):
            gamma_sum, beta_sum = carry
            for block in range(FEW):
                for tile, cost in zip((2 * block, 2 * block + 1), pack(costs[slot, rows(block)], -1.0)):
                    adjoint = adj_buf[layer, slot, tile]
                    gamma_sum = gamma_sum + cost * (adjoint * swap(start_buf[layer, slot, tile]))
                    beta_sum = beta_sum + adjoint * turn_buf[layer, slot, tile]
            return gamma_sum, beta_sum

        zero = jnp.zeros(vreg, jnp.float32)
        gamma_sum, beta_sum = lax.fori_loop(0, groups, one, (zero, zero))
        sums[1 + layer] = 2.0 * gamma_sum
        sums[1 + layers + layer] = sums[1 + layers + layer] + beta_sum

    slot_terms(last)

    @functools.partial(loop, layers // 2)
    def _(pair):
        layer = last - 2 * pair

        @functools.partial(loop, FEW)
        def _(unit):
            arrive_odd(unit, adj_recv.at[layer], adj_recv_sem.at[layer])
            cross_odd(adj_recv.at[layer], unit, -tan_buf[layer], functools.partial(unphase, layer), -tan_buf[layer - 1])
            depart_odd(layer - 1, unit, *backward_of(layer - 1))

        slot_terms(layer - 1)
        start_terms(layer, cost_other)

        @pl.when(layer > 1)
        def _():
            even = layer - 1

            @functools.partial(loop, 2)
            def _(unit):
                arrive_even(unit, adj_recv.at[even], adj_recv_sem.at[even])
                mix_slots(adj_recv.at[even], work_buf, unit, -tan_buf[even])
                cross_even(unit, -tan_buf[even], lambda slot, tiles, values: [
                    unphase(even, slot, tile, value) for tile, value in zip(tiles, values)], -tan_buf[even - 1])
                depart_even(even - 1, unit, *backward_of(even - 1))

            slot_terms(even - 1)
            start_terms(even, cost_ref)

    @functools.partial(loop, groups)
    def _(slot):
        for block in range(FEW):
            for tile, cost in zip((2 * block, 2 * block + 1), pack(cost_ref[slot, rows(block)], -1.0)):
                adj_buf[0, slot, tile] = (2.0 * cost) * swap(start_buf[0, slot, tile])

    for source, target in ((adj_buf.at[0], work_buf), (turn_buf.at[0], mixed_buf)):
        @functools.partial(loop, groups)
        def _(slot):
            for unit in range(2):
                values = butterfly([source[slot, FEW * unit + place] for place in range(FEW)], tan_buf[0])
                for place in range(FEW):
                    source[slot, FEW * unit + place] = values[place]

        for unit in range(2):
            mix_slots(source, target, unit, tan_buf[0])

    def meet(unit):
        arrive_even(unit, adj_recv.at[0], adj_recv_sem.at[0])

        def one(step, carry):
            gamma_sums, beta_sums = list(carry[:FEW]), list(carry[FEW:])
            for slot, place in [(4 * step + side, place) for side in range(4) for place in range(FEW)]:
                adjoint = adj_recv[0, slot, FEW * unit + place]
                gamma_sums[place] = gamma_sums[place] + adjoint * work_buf[slot, FEW * unit + place]
                beta_sums[place] = beta_sums[place] + adjoint * mixed_buf[slot, FEW * unit + place]
            return tuple(gamma_sums + beta_sums)

        values = lax.fori_loop(0, groups // 4, one, tuple(jnp.zeros(vreg, jnp.float32) for _ in range(2 * FEW)))
        return [(parts[0] + parts[1]) + (parts[2] + parts[3]) for parts in (values[:FEW], values[FEW:])]

    lane = lax.broadcasted_iota(jnp.int32, vreg, 1)

    def gather(terms, mine):
        for term, value in terms:
            total = jnp.sum(jnp.sum(value, axis=0, keepdims=True), axis=1, keepdims=True)
            place = jnp.logical_and(lane == max(term - 1, 0), row_index() == int(term == 0))
            mine = jnp.where(place, total, mine)
        return mine

    gamma_sum, beta_sum = meet(0)
    late = (1, 1 + layers)
    mine = gather([(term, sums[term]) for term in range(1 + 2 * layers) if term not in late], jnp.zeros(vreg, jnp.float32))
    beta_sum = beta_sum + sums[1 + layers]
    gamma_last, beta_last = meet(1)
    mine = gather([(1, gamma_sum + gamma_last), (1 + layers, beta_sum + beta_last)], mine)
    sums_mine[...] = mine
    two = pl.ds(0, 2)
    over_peers(lambda peer: copy_to(peer, sums_mine.at[two], sums_all.at[me, two], sum_sem.at[0], sum_sem.at[1]))
    drain(cost_other.at[others], cost_sem.at[0])

    @functools.partial(loop, layers)
    def _(layer):
        drain(send_buf.at[layer, others], send_sem.at[layer])
        drain(adj_send.at[layer, others], adj_send_sem.at[layer])

    drain(sums_all.at[others, two], sum_sem.at[1])
    totals = [jnp.where(slot == me, mine, sums_all[slot]) for slot in slots]
    while len(totals) > 1:
        totals = [low + high for low, high in zip(totals[0::2], totals[1::2])]
    terms_ref[...] = totals[0]

    drain(sums_all.at[others, two], sum_sem.at[0])


def finish(terms_ref, real_in, imag_in, energy_ref, grad_ref, real_ref, imag_ref, energy_buf, grad_buf, sems):
    copies = [pltpu.make_async_copy(source, target, sems.at[place]) for place, (source, target) in enumerate((
        (real_in, real_ref), (imag_in, imag_ref), (energy_buf, energy_ref), (grad_buf, grad_ref)))]
    copies[0].start()
    copies[1].start()
    grad_buf[...] = terms_ref[0, :grad_buf.shape[0]]
    energy_buf[...] = terms_ref[1, :1]
    copies[2].start()
    copies[3].start()
    for copy in copies:
        copy.wait()


def solution(mesh):
    groups = mesh.shape['qx']

    def per_device(cost_flat, phase_angles, mixer_angles):
        chunk_len = cost_flat.shape[0]
        layers = phase_angles.shape[0]
        slot_rows = chunk_len // (groups * LANES)
        assert slot_rows == TILES * HALF and layers % 2 == 0 and groups == 2 * SUBLANES
        qubits = int(math.log2(chunk_len * groups))
        slots = (groups, slot_rows, LANES)
        vreg = (SUBLANES, LANES)
        state = (groups, TILES) + vreg
        states = (layers,) + state
        f32 = jnp.float32
        vmem = pl.BlockSpec(memory_space=pltpu.VMEM)
        hbm = pl.BlockSpec(memory_space=pltpu.HBM)
        dma = pltpu.SemaphoreType.DMA
        shape_of = jax.ShapeDtypeStruct
        results = pl.pallas_call(
            functools.partial(kernel, layers, groups, qubits),
            name='qaoa',
            out_shape=[shape_of(vreg, f32), shape_of(slots, f32), shape_of(slots, f32)],
            in_specs=[hbm] * 3,
            out_specs=[vmem] * 3,
            scratch_shapes=[
                pltpu.VMEM(slots, f32),
                pltpu.SMEM((layers,), f32),
                pltpu.SMEM((layers,), f32),
                pltpu.VMEM(slots, f32),
                pltpu.VMEM((layers,) + vreg, f32),
                pltpu.VMEM((layers,) + vreg, f32),
                pltpu.VMEM(states, f32),
                pltpu.VMEM(states, f32),
                pltpu.VMEM(states, f32),
                pltpu.VMEM(states, f32),
                pltpu.VMEM(state, f32),
                pltpu.VMEM(state, f32),
                pltpu.VMEM(states, f32),
                pltpu.VMEM(states, f32),
                pltpu.VMEM(states, f32),
                pltpu.VMEM(states, f32),
                pltpu.VMEM(states, f32),
                pltpu.VMEM((1 + 2 * layers,) + vreg, f32),
                pltpu.VMEM(vreg, f32),
                pltpu.VMEM((groups,) + vreg, f32),
                dma((layers,)), dma((layers, 1 + FEW)), dma((layers,)), dma((layers, 1 + FEW)),
                dma((2,)), dma((2,)), dma((3,)),
            ],
            compiler_params=pltpu.CompilerParams(
                collective_id=0, has_side_effects=True, vmem_limit_bytes=34 * 1024 * 1024),
        )(*(pltpu.with_memory_space_constraint(value, pltpu.HBM)
            for value in (cost_flat.reshape(slots), phase_angles, mixer_angles)))
        energy, grad, real, imag = pl.pallas_call(
            finish,
            name='finish',
            out_shape=[shape_of((1,), f32), shape_of((2 * layers,), f32), shape_of(slots, f32), shape_of(slots, f32)],
            in_specs=[vmem] * 3,
            out_specs=[hbm] * 4,
            scratch_shapes=[pltpu.VMEM((1,), f32), pltpu.VMEM((2 * layers,), f32), dma((4,))],
            compiler_params=pltpu.CompilerParams(vmem_limit_bytes=2 * 1024 * 1024),
        )(*results)
        return energy, grad, real.reshape(chunk_len), imag.reshape(chunk_len)

    return jax.shard_map(
        per_device, mesh=mesh, in_specs=(P(('inst', 'qx')), P(), P()),
        out_specs=(P('inst'), P('inst'), P(('inst', 'qx')), P(('inst', 'qx'))), check_vma=False)
```
